8 devices in a mesh: dp: 2 (over z, y), tp: 4 (over x, core).
Axes of the slice: x: 2, y: 2, z: 1, core: 2. Of those that a mesh axis runs over, the one named last changes fastest.
Arguments:
- tokens: int32 [64, 256], P('dp'), parts along dimension 0
- attn_mask: int32 [64, 256], P('dp'), parts along dimension 0
- emb_table: bfloat16 [50272, 768], P('tp')
- pos_table: bfloat16 [2050, 768], replicated
- ln1_gain: bfloat16 [768], replicated
- ln1_shift: bfloat16 [768], replicated
- w_qkv: bfloat16 [3, 768, 12, 64], P(None, None, 'tp')
- b_qkv: bfloat16 [3, 12, 64], P(None, 'tp')
- w_out: bfloat16 [12, 64, 768], P('tp')
- b_out: bfloat16 [768], replicated
- ln2_gain: bfloat16 [768], replicated
- ln2_shift: bfloat16 [768], replicated
- w_fc1: bfloat16 [768, 3072], P(None, 'tp')
- b_fc1: bfloat16 [3072], P('tp')
- w_fc2: bfloat16 [3072, 768], P('tp')
- b_fc2: bfloat16 [768], replicated
- grad_y: bfloat16 [64, 256, 768], P('dp', 'tp'), parts along dimension 0
Outputs:
- output 1: bfloat16 [64, 256, 768], P('dp', 'tp'), parts along dimension 0
- output 2: float32 [100544, 768], P(('dp', 'tp')), parts along dimension 0
- output 3: float32 [4100, 768], P('dp'), parts along dimension 0
- output 4: float32 [1536], P('dp'), parts along dimension 0
- output 5: float32 [1536], P('dp'), parts along dimension 0
- output 6: float32 [6, 768, 12, 64], P('dp', None, 'tp'), parts along dimension 0
- output 7: float32 [6, 12, 64], P('dp', 'tp'), parts along dimension 0
- output 8: float32 [24, 64, 768], P(('dp', 'tp')), parts along dimension 0
- output 9: float32 [1536], P('dp'), parts along dimension 0
- output 10: float32 [1536], P('dp'), parts along dimension 0
- output 11: float32 [1536], P('dp'), parts along dimension 0
- output 12: float32 [1536, 3072], P('dp', 'tp'), parts along dimension 0
- output 13: float32 [6144], P(('dp', 'tp')), parts along dimension 0
- output 14: float32 [6144, 768], P(('dp', 'tp')), parts along dimension 0
- output 15: float32 [1536], P('dp'), parts along dimension 0
There are 2 independent parts. The reference program is written for one: setup_inputs(seed, part) draws one part's arguments, and reference() takes and returns one part's arrays. A program takes and returns all parts, laid end to end along the dimension named above; an argument that names none is the same for every part.
All inputs are finite; a program needn't handle non-finite values.
Results may differ from the reference program's by a relative error of at most 0.02.
Values are sent between devices in bfloat16 or wider.
A program may use at most 1 GiB of HBM per device.

```python
import math
import jax
import jax.numpy as jnp
from jax import lax

BATCH_ROWS = 32
SEQ_LEN = 256
D_MODEL = 768
NUM_HEADS = 12
FF_DIM = 3072
VOCAB_SIZE = 50272
VOCAB_PAD = 50272
POS_ROWS = 2050
HEAD_DIM = D_MODEL // NUM_HEADS
Q_SCALE = 1.0 / math.sqrt(HEAD_DIM)
LN_EPS = 1e-5
NEG_BIG = -1e30


def setup_inputs(seed: int = 0, part: int = 0) -> dict:
    base_key = jax.random.key(seed)
    part_key = jax.random.fold_in(base_key, part)
    id_keys = jax.random.split(part_key, 5)
    pick_wide = jax.random.randint(id_keys[0], (BATCH_ROWS, SEQ_LEN), 0, 2)
    wide_ids = jax.random.randint(id_keys[1], (BATCH_ROWS, SEQ_LEN), 0, VOCAB_SIZE)
    common_ids = jax.random.randint(id_keys[2], (BATCH_ROWS, SEQ_LEN), 0, 2048)
    tokens = jnp.where(pick_wide == 1, wide_ids, common_ids).astype(jnp.int32)
    pad_counts = jax.random.randint(id_keys[3], (BATCH_ROWS,), 0, SEQ_LEN // 2 + 1)
    pad_counts = pad_counts.at[BATCH_ROWS - 1].set(SEQ_LEN // 2)
    attn_mask = (jnp.arange(SEQ_LEN)[None, :] >= pad_counts[:, None]).astype(jnp.int32)
    weight_keys = jax.random.split(base_key, 14)

    def normal_draw(draw_index, draw_shape):
        return jax.random.normal(weight_keys[draw_index], draw_shape, jnp.float32)

    d_scale = 1.0 / math.sqrt(D_MODEL)
    qkv_gain = jnp.array([1.4, 1.4, 1.0], jnp.float32)[:, None, None, None]
    fc1_draw = normal_draw(11, (FF_DIM,))
    return {
        'tokens': tokens,
        'attn_mask': attn_mask,
        'emb_table': normal_draw(0, (VOCAB_PAD, D_MODEL)).astype(jnp.bfloat16),
        'pos_table': (0.7 * normal_draw(1, (POS_ROWS, D_MODEL))).astype(jnp.bfloat16),
        'ln1_gain': (1.0 + 0.3 * normal_draw(2, (D_MODEL,))).astype(jnp.bfloat16),
        'ln1_shift': (0.5 * normal_draw(3, (D_MODEL,))).astype(jnp.bfloat16),
        'w_qkv': (normal_draw(4, (3, D_MODEL, NUM_HEADS, HEAD_DIM)) * qkv_gain * d_scale).astype(jnp.bfloat16),
        'b_qkv': (0.3 * normal_draw(5, (3, NUM_HEADS, HEAD_DIM))).astype(jnp.bfloat16),
        'w_out': (2.0 * d_scale * normal_draw(6, (NUM_HEADS, HEAD_DIM, D_MODEL))).astype(jnp.bfloat16),
        'b_out': (0.5 * normal_draw(7, (D_MODEL,))).astype(jnp.bfloat16),
        'ln2_gain': (1.0 + 0.3 * normal_draw(8, (D_MODEL,))).astype(jnp.bfloat16),
        'ln2_shift': (0.5 * normal_draw(9, (D_MODEL,))).astype(jnp.bfloat16),
        'w_fc1': (d_scale * normal_draw(10, (D_MODEL, FF_DIM))).astype(jnp.bfloat16),
        'b_fc1': (jnp.where(fc1_draw > 0, 3.0, -3.0) + 0.3 * fc1_draw).astype(jnp.bfloat16),
        'w_fc2': ((0.4 / math.sqrt(FF_DIM)) * normal_draw(12, (FF_DIM, D_MODEL))).astype(jnp.bfloat16),
        'b_fc2': (0.5 * normal_draw(13, (D_MODEL,))).astype(jnp.bfloat16),
        'grad_y': jax.random.normal(id_keys[4], (BATCH_ROWS, SEQ_LEN, D_MODEL), jnp.float32).astype(jnp.bfloat16),
    }


def layer_norm(hidden, ln_gain, ln_shift):
    hidden32 = hidden.astype(jnp.float32)
    centered = hidden32 - jnp.mean(hidden32, axis=-1, keepdims=True)
    variance = jnp.mean(jnp.square(centered), axis=-1, keepdims=True)
    scaled = centered * lax.rsqrt(variance + LN_EPS)
    return (scaled * ln_gain.astype(jnp.float32) + ln_shift.astype(jnp.float32)).astype(jnp.bfloat16)


def block_forward(tok_part, pos_part, ln1_gain, ln1_shift, w_qkv, b_qkv, w_out, b_out, ln2_gain, ln2_shift, w_fc1, b_fc1, w_fc2, b_fc2, allowed):
    hidden0 = (tok_part + pos_part).astype(jnp.bfloat16)
    normed1 = layer_norm(hidden0, ln1_gain, ln1_shift)
    qkv_proj = jnp.einsum('bsd,tdhe->tbshe', normed1.astype(jnp.float32), w_qkv.astype(jnp.float32)) + b_qkv.astype(jnp.float32)[:, None, None]
    query_rows = (qkv_proj[0] * Q_SCALE).astype(jnp.bfloat16)
    key_rows = qkv_proj[1].astype(jnp.bfloat16)
    value_rows = qkv_proj[2].astype(jnp.bfloat16)
    scores = jnp.einsum('bqhe,bkhe->bhqk', query_rows.astype(jnp.float32), key_rows.astype(jnp.float32))
    attn_probs = jax.nn.softmax(jnp.where(allowed, scores, NEG_BIG), axis=-1)
    context = jnp.einsum('bhqk,bkhe->bqhe', attn_probs.astype(jnp.bfloat16).astype(jnp.float32), value_rows.astype(jnp.float32)).astype(jnp.bfloat16)
    attn_sum = jnp.einsum('bqhe,hed->bqd', context.astype(jnp.float32), w_out.astype(jnp.float32))
    hidden1 = (hidden0.astype(jnp.float32) + attn_sum + b_out.astype(jnp.float32)).astype(jnp.bfloat16)
    normed2 = layer_norm(hidden1, ln2_gain, ln2_shift)
    mlp_inner = jax.nn.relu(jnp.einsum('bsd,df->bsf', normed2.astype(jnp.float32), w_fc1.astype(jnp.float32)) + b_fc1.astype(jnp.float32)).astype(jnp.bfloat16)
    mlp_sum = jnp.einsum('bsf,fd->bsd', mlp_inner.astype(jnp.float32), w_fc2.astype(jnp.float32))
    return (hidden1.astype(jnp.float32) + mlp_sum + b_fc2.astype(jnp.float32)).astype(jnp.bfloat16)


def reference(tokens, attn_mask, emb_table, pos_table, ln1_gain, ln1_shift, w_qkv, b_qkv, w_out, b_out, ln2_gain, ln2_shift, w_fc1, b_fc1, w_fc2, b_fc2, grad_y):
    positions = jnp.cumsum(attn_mask, axis=1) * attn_mask + 1
    tok_part = jnp.take(emb_table, tokens, axis=0).astype(jnp.float32)
    pos_part = jnp.take(pos_table, positions, axis=0).astype(jnp.float32)
    seq_index = jnp.arange(SEQ_LEN)
    causal = (seq_index[:, None] >= seq_index[None, :])[None, None]
    diagonal = (seq_index[:, None] == seq_index[None, :])[None, None]
    allowed = causal & ((attn_mask[:, None, None, :] == 1) | diagonal)

    def forward(tok_in, pos_in, *weights):
        return block_forward(tok_in, pos_in, *weights, allowed)

    out_rows, pullback = jax.vjp(forward, tok_part, pos_part, ln1_gain, ln1_shift, w_qkv, b_qkv, w_out, b_out, ln2_gain, ln2_shift, w_fc1, b_fc1, w_fc2, b_fc2)
    grad_list = pullback(grad_y)
    d_hidden0 = grad_list[0].reshape(-1, D_MODEL)
    d_emb = jax.ops.segment_sum(d_hidden0, tokens.reshape(-1), num_segments=VOCAB_PAD)
    d_pos = jax.ops.segment_sum(d_hidden0, positions.reshape(-1), num_segments=POS_ROWS)
    return (out_rows, d_emb, d_pos, grad_list[2].astype(jnp.float32), grad_list[3].astype(jnp.float32), grad_list[4].astype(jnp.float32), grad_list[5].astype(jnp.float32), grad_list[6].astype(jnp.float32), grad_list[7].astype(jnp.float32), grad_list[8].astype(jnp.float32), grad_list[9].astype(jnp.float32), grad_list[10].astype(jnp.float32), grad_list[11].astype(jnp.float32), grad_list[12].astype(jnp.float32), grad_list[13].astype(jnp.float32))
```

```python
import math
import jax
import jax.numpy as jnp
from jax import lax
from jax.experimental import pallas as pl
from jax.experimental.pallas import tpu as pltpu
from jax.sharding import PartitionSpec as P

LN_EPS = 1e-5
NEG_BIG = -1e30
LANE = 128
VMEM = 62 * 2**20
UNROLL = 4
TP, X, CORE, HALVES, QKV = 4, 2, 1, 2, 3
ROWS = 0
NN, NT, TN = ((1,), (0,)), ((1,), (1,)), ((0,), (0,))
SUB = 8
BATCH = 16
F32 = jnp.float32
BF16 = jnp.bfloat16


def swap(value, step):
    return lax.ppermute(value, 'tp', [(i, i ^ step) for i in range(4)])


def xor_order(value, rank):
    value = jnp.where((rank & 2) > 0, jnp.concatenate([value[2:], value[:2]]), value)
    flipped = jnp.stack([value[1], value[0], value[3], value[2]])
    return jnp.where((rank & 1) > 0, flipped, value)


def dot(a, b, dims, out=F32):
    return lax.dot_general(a, b, (dims, ((), ())), preferred_element_type=F32).astype(out)


def ln_stats(hidden):
    hidden32 = hidden.astype(F32)
    centered = hidden32 - jnp.mean(hidden32, axis=-1, keepdims=True)
    variance = jnp.mean(jnp.square(centered), axis=-1, keepdims=True)
    inv = lax.rsqrt(variance + LN_EPS)
    return centered * inv, inv


def ln_forward(hidden, gain, shift):
    scaled, _ = ln_stats(hidden)
    return (scaled * gain.astype(F32) + shift.astype(F32)).astype(BF16)


def ln_backward(hidden, gain, d_out):
    scaled, inv = ln_stats(hidden)
    d_out = d_out.astype(F32)
    d_gain = jnp.sum(d_out * scaled, axis=0)
    d_shift = jnp.sum(d_out, axis=0)
    d_scaled = d_out * gain.astype(F32)
    mean_d = jnp.mean(d_scaled, axis=-1, keepdims=True)
    mean_ds = jnp.mean(d_scaled * scaled, axis=-1, keepdims=True)
    return (d_scaled - mean_d - scaled * mean_ds) * inv, d_gain, d_shift


def half_of(pair, keep):
    return jnp.where(keep, pair, jnp.zeros_like(pair))


def softmax(scores, allowed, axis):
    scores = jnp.where(allowed, scores, NEG_BIG)
    weights = jnp.exp(scores - jnp.max(scores, axis=axis, keepdims=True))
    return weights * (1.0 / jnp.sum(weights, axis=axis, keepdims=True))


def pair_offsets(width):
    span = width // 6
    return [(half * 3 * span + j, half * 3 * span + span + j, half * 3 * span + 2 * span + j, half * span + j)
            for half in range(2) for j in range(0, span, LANE)]


def allowed_of(mask_ref):
    return mask_ref[0] > 0


def attn_fwd_kernel(mask_ref, qkv_ref, ctx_ref):
    rows, width = mask_ref.shape[1], qkv_ref.shape[-1]
    allowed = allowed_of(mask_ref)
    low = lax.broadcasted_iota(jnp.int32, (rows, LANE), 1) < 64

    def take(start):
        return qkv_ref[:, 0, :, start:start + LANE].reshape(rows, LANE)

    for qo, ko, vo, co in pair_offsets(width):
        q, k, v = take(qo), take(ko), take(vo)
        parts = [dot(softmax(dot(half_of(q, keep), k, NT), allowed, -1).astype(BF16), v, NN) for keep in (low, ~low)]
        ctx = jnp.where(low, parts[0], parts[1]).astype(BF16)
        ctx_ref[:, 0, :, co:co + LANE] = ctx.reshape(ctx_ref.shape[0], -1, LANE)


def attn_bwd_kernel(q_scale, mask_ref, qkv_ref, dctx_ref, dqkv_ref, bias_ref):
    rows, width = mask_ref.shape[1], qkv_ref.shape[-1]
    allowed = allowed_of(mask_ref)
    low = lax.broadcasted_iota(jnp.int32, (rows, LANE), 1) < 64

    @pl.when(pl.program_id(0) == 0)
    def _():
        bias_ref[...] = jnp.zeros_like(bias_ref)

    def take(ref, start):
        return ref[:, 0, :, start:start + LANE].reshape(rows, LANE)

    def put(start, value):
        bias_ref[0:1, start:start + LANE] += jnp.sum(value, axis=ROWS, keepdims=True)
        dqkv_ref[:, 0, :, start:start + LANE] = value.astype(BF16).reshape(dqkv_ref.shape[0], -1, LANE)

    for qo, ko, vo, co in pair_offsets(width):
        q, k, v = take(qkv_ref, qo), take(qkv_ref, ko), take(qkv_ref, vo)
        dc = take(dctx_ref, co)
        parts = []
        for keep in (low, ~low):
            probs = softmax(dot(k, half_of(q, keep), NT), allowed, 0)
            d_probs = dot(v, half_of(dc, keep), NT)
            d_scores = (probs * (d_probs - jnp.sum(d_probs * probs, axis=ROWS, keepdims=True))).astype(BF16)
            parts.append((dot(d_scores, k, TN) * q_scale, dot(d_scores, q, NN), dot(probs.astype(BF16), dc, NN)))
        for start, a, b in zip((qo, ko, vo), *parts):
            put(start, jnp.where(low, a, b))


def seq_spec(width, seq_local, chunk=None):
    if chunk is None:
        return pl.BlockSpec((4, 1, seq_local, width), lambda s: (0, s, 0, 0))
    return pl.BlockSpec((None, 4, 1, seq_local, width), lambda s: (chunk, 0, s, 0, 0))


def mask_spec(seq, chunk, n_seq):
    return pl.BlockSpec((1, seq, seq), lambda s: (chunk * n_seq + s, 0, 0))


def attn_forward(allowed, qkv, chunk):
    _, n_seq, seq_local, width = qkv.shape
    seq = 4 * seq_local
    return pl.pallas_call(
        attn_fwd_kernel, grid=(n_seq,),
        out_shape=jax.ShapeDtypeStruct((4, n_seq, seq_local, width // 3), BF16),
        in_specs=[mask_spec(seq, chunk, n_seq), seq_spec(width, seq_local)],
        out_specs=seq_spec(width // 3, seq_local),
        cost_estimate=pl.CostEstimate(flops=n_seq * 12 * seq * seq * 512, bytes_accessed=qkv.size * 3, transcendentals=ROWS),
        name='attn_fwd')(allowed, qkv)


def attn_backward(allowed, qkv, d_ctx, chunk, q_scale):
    _, n_seq, seq_local, width = qkv.shape
    seq = 4 * seq_local
    return pl.pallas_call(
        lambda *refs: attn_bwd_kernel(q_scale, *refs), grid=(n_seq,),
        out_shape=[jax.ShapeDtypeStruct(qkv.shape, BF16), jax.ShapeDtypeStruct((8, width), F32)],
        in_specs=[mask_spec(seq, chunk, n_seq), seq_spec(width, seq_local), seq_spec(width // 3, seq_local, chunk)],
        out_specs=[seq_spec(width, seq_local), pl.BlockSpec((8, width), lambda s: (0, 0))],
        cost_estimate=pl.CostEstimate(flops=n_seq * 12 * seq * seq * 1280, bytes_accessed=qkv.size * 6, transcendentals=ROWS),
        name='attn_bwd')(allowed, qkv, d_ctx)


def group_rows(lanes):
    return -(-(lanes * (SUB + 1)) // SUB) * SUB


def row_slice(start, lanes):
    return pl.ds(start, lanes, stride=SUB + 1)


def tile_loop(rows, lanes, body):
    def step(t, _):
        for j in range(lanes):
            body(pl.ds(pl.multiple_of(t * 2 * SUB, 2 * SUB), 2 * SUB), [(2 * t + h) * group_rows(lanes) + j * (SUB + 1) for h in range(2)], pl.ds(j * LANE, LANE))
        return 0

    lax.fori_loop(0, rows // (2 * SUB), step, 0, unroll=2)


def spread(dst_ref, start, src_ref):
    def body(rows, groups, cols):
        piece = src_ref[rows, cols].astype(F32)
        for h, at in enumerate(groups):
            dst_ref[pl.ds(start + at, SUB), :] = piece[h * SUB:(h + 1) * SUB]

    tile_loop(src_ref.shape[0], src_ref.shape[1] // LANE, body)


def collect(dst_ref, src_ref):
    def body(rows, groups, cols):
        dst_ref[rows, cols] = jnp.concatenate([src_ref[pl.ds(at, SUB), :] for at in groups]).astype(dst_ref.dtype)

    tile_loop(dst_ref.shape[0], dst_ref.shape[1] // LANE, body)


def placed(ids, lanes):
    return (ids // SUB) * group_rows(lanes) + ids % SUB


def gather_kernel(first, block, at_ref, table_ref, *refs):
    outs, (held_ref, rows_ref) = refs[:-2], refs[-2:]
    lanes = table_ref.shape[1] // LANE
    group = group_rows(lanes)
    step = pl.program_id(0)
    per = (pl.num_programs(0) - first) // len(outs)

    @pl.when(step < first)
    def _():
        held_ref[held_ref.shape[0] - group:, :] = jnp.zeros((group, LANE), F32)
        spread(held_ref, step * (table_ref.shape[0] // SUB * group), table_ref)

    @pl.when(step >= first)
    def _():
        def take(batch, _):
            for i in range(BATCH):
                row = held_ref[row_slice(at_ref[(step - first) * block + batch * BATCH + i], lanes), :]
                rows_ref[row_slice((batch * (BATCH // SUB) + i // SUB) * group + i % SUB, lanes), :] = row
            return 0

        lax.fori_loop(0, block // BATCH, take, 0)
        for k, out in enumerate(outs):
            pl.when((step - first) // per == k)(lambda out=out: collect(out, rows_ref))


def gather(table, ids, owned, n_out, block=512, table_block=1024):
    vocab_local, d = table.shape
    first, lanes, per = -(-vocab_local // table_block), d // LANE, ids.size // (n_out * block)
    at = placed(jnp.where(owned, ids, first * table_block), lanes)
    group = group_rows(lanes)

    def out_spec(k):
        return pl.BlockSpec((block, d), lambda s, *_: (jnp.clip(s - first - k * per, 0, per - 1), 0))

    return pl.pallas_call(
        lambda *refs: gather_kernel(first, block, *refs),
        grid_spec=pltpu.PrefetchScalarGridSpec(
            num_scalar_prefetch=1, grid=(first + n_out * per,),
            in_specs=[pl.BlockSpec((table_block, d), lambda s, *_: (jnp.minimum(s, first - 1), 0))],
            out_specs=[out_spec(k) for k in range(n_out)],
            scratch_shapes=[pltpu.VMEM(((first * table_block // SUB + 1) * group, LANE), F32), pltpu.VMEM((block // SUB * group, LANE), F32)]),
        out_shape=[jax.ShapeDtypeStruct((per * block, d), BF16)] * n_out,
        compiler_params=pltpu.CompilerParams(vmem_limit_bytes=VMEM),
        name='emb_gather')(at.reshape(-1), table)


def scatter_kernel(n_src, n_tiles, block, out_tiles, ids_ref, repeat_ref, *refs):
    srcs, (out_ref, acc_ref, rows_ref, stage_ref, sem) = refs[:n_src], refs[n_src:]
    step = pl.program_id(0)
    lanes = stage_ref.shape[-1] // LANE
    group = group_rows(lanes)
    per_src = pl.num_programs(0) // n_src

    @pl.when(step == 0)
    def _():
        def clear(i, _):
            acc_ref[pl.ds(pl.multiple_of(i * group, SUB), group), :] = jnp.zeros((group, LANE), F32)
            return 0

        lax.fori_loop(0, acc_ref.shape[0] // group, clear, 0, unroll=UNROLL)

    for k, src in enumerate(srcs):
        pl.when(step // per_src == k)(lambda src=src: spread(rows_ref, 0, src))

    def add(batch, _):
        first = step * block + batch * BATCH
        tiles = BATCH // SUB
        slots = [acc_ref.at[row_slice(ids_ref[first + i], lanes), :] for i in range(BATCH)]
        rows = [rows_ref.at[row_slice((batch * tiles + i // SUB) * group + i % SUB, lanes), :] for i in range(BATCH)]
        repeats = repeat_ref[step * (block // BATCH) + batch]

        @pl.when(repeats == 0)
        def _():
            sums = [slot[...] + row[...] for slot, row in zip(slots, rows)]
            for slot, total in zip(slots, sums):
                slot[...] = total

        @pl.when(repeats != 0)
        def _():
            for slot, row in zip(slots, rows):
                slot[...] += row[...]

        return 0

    lax.fori_loop(0, block // BATCH, add, 0)

    @pl.when(step == pl.num_programs(0) - 1)
    def _():
        n_out, rest = divmod(n_tiles, out_tiles)

        def copy(start, slot, size):
            return pltpu.make_async_copy(stage_ref.at[slot, pl.ds(0, size)], out_ref.at[pl.ds(start, size)], sem.at[slot])

        def stage(start, slot, size):
            def move(t, _):
                for j in range(lanes):
                    stage_ref[slot, t, :, pl.ds(j * LANE, LANE)] = acc_ref[pl.ds((start + t) * group + j * (SUB + 1), SUB), :]
                return 0

            lax.fori_loop(0, size, move, 0, unroll=UNROLL if size % UNROLL == 0 else 1)

        def flush(i, _):
            slot = lax.rem(i, 2)

            @pl.when(i >= 2)
            def _():
                copy((i - 2) * out_tiles, slot, out_tiles).wait()

            stage(i * out_tiles, slot, out_tiles)
            copy(i * out_tiles, slot, out_tiles).start()
            return 0

        lax.fori_loop(0, n_out, flush, 0)
        copy((n_out - 2) * out_tiles, n_out % 2, out_tiles).wait()
        if rest:
            stage(n_out * out_tiles, n_out % 2, rest)
            copy(n_out * out_tiles, n_out % 2, rest).start()
        copy((n_out - 1) * out_tiles, (n_out - 1) % 2, out_tiles).wait()
        if rest:
            copy(n_out * out_tiles, n_out % 2, rest).wait()


def repeats(ids, vocab_local):
    batch = ids.reshape(-1, BATCH)
    same = jnp.zeros(batch.shape[:1], bool)
    for i in range(1, BATCH):
        same |= jnp.any((batch[:, i:] == batch[:, :-i]) & (batch[:, i:] < vocab_local), axis=1)
    return same.astype(jnp.int32)


def scatter(ids, repeat, srcs, vocab_local, block=512):
    rows, d = srcs[0].shape
    n_src = len(srcs)
    n_tiles = vocab_local // SUB
    out_tiles = 64
    per = rows // block
    lanes = d // 128
    group = group_rows(lanes)

    def spec(k):
        return pl.BlockSpec((block, d), lambda s, *_: (jnp.clip(s - k * per, 0, per - 1), 0))

    out = pl.pallas_call(
        lambda *r: scatter_kernel(n_src, n_tiles, block, out_tiles, *r),
        grid_spec=pltpu.PrefetchScalarGridSpec(num_scalar_prefetch=2, grid=(n_src * per,),
            in_specs=[spec(k) for k in range(n_src)], out_specs=pl.BlockSpec(memory_space=pl.ANY),
            scratch_shapes=[pltpu.VMEM(((n_tiles + 1) * group, 128), F32), pltpu.VMEM((block // SUB * group, 128), F32),
                            pltpu.VMEM((2, out_tiles, SUB, d), F32), pltpu.SemaphoreType.DMA((2,))]),
        out_shape=jax.ShapeDtypeStruct((n_tiles, SUB, d), F32),
        compiler_params=pltpu.CompilerParams(vmem_limit_bytes=VMEM),
        cost_estimate=pl.CostEstimate(flops=50 * 10**9, bytes_accessed=4 * vocab_local * d, transcendentals=ROWS),
        name='emb_scatter')(placed(ids, lanes), repeat, *srcs)
    return out.reshape(vocab_local, d)


def ff_slices(width, block=512):
    return [pl.ds(i * block, block) for i in range(width // block)]


def zero_first(*refs):
    @pl.when(pl.program_id(0) == 0)
    def _():
        for ref in refs:
            ref[...] = jnp.zeros_like(ref)


def at_last(ref, total_ref):
    @pl.when(pl.program_id(0) == pl.num_programs(0) - 1)
    def _():
        ref[...] = total_ref[...].astype(ref.dtype)


def add_row(ref, index, value, cols=slice(None)):
    ref[pl.ds(index, 1), cols] += jnp.sum(value, axis=ROWS, keepdims=True)


def chunk_tile(refs):
    tile = refs[0][...]
    for c, ref in enumerate(refs):
        tile = jnp.where(pl.program_id(0) * len(refs) >= c * pl.num_programs(0), ref[...], tile)
    return tile


def mlp_forward_kernel(*refs):
    h0_refs, ctx_refs, refs = refs[:2], refs[2:4], refs[4:]
    g_ref, wout_ref, w1n_ref, w1f_ref, w2n_ref, w2f_ref, vec_ref, b1_ref = refs[:8]
    out_ref, h1_ref, n2_ref, dpren_ref, dpref_ref, dw2n_ref, dw2f_ref, db1_ref, sum_ref, far_ref = refs[8:]
    zero_first(dw2n_ref, far_ref, db1_ref, sum_ref)
    b_out, gain, shift, b_fc2 = (vec_ref[i:i + 1] for i in range(4))
    grad = g_ref[...]
    hidden1 = (chunk_tile(h0_refs).astype(F32) + dot(chunk_tile(ctx_refs), wout_ref[...], NN) + b_out).astype(BF16)
    h1_ref[...] = hidden1
    scaled, _ = ln_stats(hidden1)
    normed2 = (scaled * gain + shift).astype(BF16)
    n2_ref[...] = normed2
    total = hidden1.astype(F32) + b_fc2
    halves = ((w1n_ref, w2n_ref, dpren_ref, dw2n_ref), (w1f_ref, w2f_ref, dpref_ref, far_ref))
    for half, (w1_ref, w2_ref, dpre_ref, dw2_ref) in enumerate(halves):
        for cols in ff_slices(w1_ref.shape[0]):
            inner = dot(normed2, w1_ref[cols, :], NT) + b1_ref[half:half + 1, cols]
            inner = jnp.maximum(inner, 0.0).astype(BF16)
            total += dot(inner, w2_ref[cols, :], NN)
            dw2_ref[cols, :] += dot(inner, grad, TN)
            d_pre = jnp.where(inner > 0, dot(grad, w2_ref[cols, :], NT), 0.0)
            add_row(db1_ref, half, d_pre, cols)
            dpre_ref[:, cols] = d_pre.astype(BF16)
    out_ref[...] = total.astype(BF16)
    add_row(sum_ref, 0, grad.astype(F32))
    at_last(dw2f_ref, far_ref)


def mlp_backward_kernel(*refs):
    ctx_refs, refs = refs[:2], refs[2:]
    dpren_ref, dpref_ref, n2_ref, h1_ref, g_ref, w1n_ref, w1f_ref, wout_ref, gain_ref = refs[:9]
    dh1_ref, dctx_ref, dw1n_ref, dw1f_ref, dwon_ref, dwof_ref, sum_ref, w1far_ref, wofar_ref = refs[9:]
    zero_first(dw1n_ref, dwon_ref, w1far_ref, wofar_ref, sum_ref)
    normed2 = n2_ref[...]
    d_norm2 = jnp.zeros(normed2.shape, F32)
    for w1_ref, dpre_ref, dw1_ref in ((w1n_ref, dpren_ref, dw1n_ref), (w1f_ref, dpref_ref, w1far_ref)):
        for cols in ff_slices(w1_ref.shape[0]):
            d_pre = dpre_ref[:, cols]
            d_norm2 += dot(d_pre, w1_ref[cols, :], NN)
            dw1_ref[cols, :] += dot(d_pre, normed2, TN)
    d_norm2 = d_norm2.astype(BF16).astype(F32)
    scaled, inv = ln_stats(h1_ref[...])
    add_row(sum_ref, 0, d_norm2 * scaled)
    add_row(sum_ref, 1, d_norm2)
    d_scaled = d_norm2 * gain_ref[...]
    mean_d = jnp.mean(d_scaled, axis=-1, keepdims=True)
    mean_ds = jnp.mean(d_scaled * scaled, axis=-1, keepdims=True)
    d_hidden1 = (g_ref[...].astype(F32) + (d_scaled - mean_d - scaled * mean_ds) * inv).astype(BF16)
    dh1_ref[...] = d_hidden1
    add_row(sum_ref, 2, d_hidden1.astype(F32))
    context = chunk_tile(ctx_refs)
    half = dwon_ref.shape[0]
    dwon_ref[...] += dot(context[:, :half], d_hidden1, TN)
    wofar_ref[...] += dot(context[:, half:], d_hidden1, TN)
    dctx_ref[...] = dot(d_hidden1, wout_ref[...], NT).astype(BF16)
    at_last(dw1f_ref, w1far_ref)
    at_last(dwof_ref, wofar_ref)


TILE = 512


def row_spec(array):
    return pl.BlockSpec((TILE, array.shape[1]), lambda s: (s, 0))


def chunk_specs(arrays):
    per = arrays[0].shape[0] // TILE
    return [pl.BlockSpec((TILE, a.shape[1]), lambda s, c=c: (jnp.clip(s - c * per, 0, per - 1), 0)) for c, a in enumerate(arrays)]


def whole_spec(array):
    return pl.BlockSpec(array.shape, lambda s: (0,) * len(array.shape), pipeline_mode=pl.Buffered(1))


def fused_call(kernel, chunked, tiled, whole, tiled_out, whole_out, scratch, flops):
    rows = tiled[0].shape[0]
    return pl.pallas_call(
        kernel, grid=(rows // TILE,),
        in_specs=sum([chunk_specs(a) for a in chunked], []) + [row_spec(a) for a in tiled] + [whole_spec(a) for a in whole],
        out_shape=tiled_out + whole_out,
        out_specs=[row_spec(a) for a in tiled_out] + [whole_spec(a) for a in whole_out],
        scratch_shapes=[pltpu.VMEM(a, F32) for a in scratch],
        compiler_params=pltpu.CompilerParams(vmem_limit_bytes=VMEM),
        cost_estimate=pl.CostEstimate(flops=flops, bytes_accessed=10**8, transcendentals=ROWS),
    )(*sum(chunked, []), *tiled, *whole)


def mlp_forward(hidden0, context, grad, wout, w1, w2, vectors, b1):
    rows, d = grad.shape
    ff = w1[0].shape[0]
    like = jax.ShapeDtypeStruct
    tiled_out = [like((rows, d), BF16)] * 3 + [like((rows, ff), BF16)] * 2
    whole_out = [like((ff, d), F32), like((ff, d), BF16), like((SUB, ff), F32), like((SUB, d), F32)]
    return fused_call(mlp_forward_kernel, [hidden0, context], [grad], [wout, *w1, *w2, vectors, b1],
                      tiled_out, whole_out, [(ff, d)], 2 * rows * d * (d + 8 * ff))


def mlp_backward(context, d_pre, normed2, hidden1, grad, w1, wout, gain):
    rows, d = grad.shape
    ff = w1[0].shape[0]
    like = jax.ShapeDtypeStruct
    whole_out = [like((ff, d), F32), like((ff, d), BF16), like((d // 2, d), F32), like((d // 2, d), BF16), like((SUB, d), F32)]
    return fused_call(mlp_backward_kernel, [context], [*d_pre, normed2, hidden1, grad], [*w1, wout, gain],
                      [like((rows, d), BF16)] * 2, whole_out, [(ff, d), (d // 2, d)], 2 * rows * d * (2 * d + 4 * ff))


def fetch(own, y_rank):
    half = own.shape[0] // 2
    mine = swap(lax.dynamic_slice_in_dim(own, y_rank * half, half), 2)
    other = lax.ppermute(mine, 'dp', [(0, 1), (1, 0)])
    first = y_rank == 0
    far = jnp.concatenate([jnp.where(first, mine, other), jnp.where(first, other, mine)])
    near = jnp.stack([own, far])
    return near, swap(near, 1)


def solution(mesh):
    def device_body(tokens, attn_mask, emb_local, pos_table, ln1_gain, ln1_shift, w_qkv, b_qkv, w_out, b_out, ln2_gain, ln2_shift, w_fc1, b_fc1, w_fc2, b_fc2, grad_y):
        vocab_local, d_model = emb_local.shape
        n_all, seq = tokens.shape
        n_seq, seq_local = n_all // TP, seq // TP
        local_heads, e = w_qkv.shape[2:]
        n_heads = 4 * local_heads
        rows = n_seq * seq
        n_chunk = 2
        c_seq, c_rows = n_seq // n_chunk, rows // n_chunk
        hidden = local_heads * e
        ff_local = w_fc2.shape[0]
        q_scale = 1.0 / math.sqrt(e)
        rank = lax.axis_index('tp')
        y_rank = lax.axis_index('dp')
        barrier = lax.optimization_barrier

        qkv_rows = w_qkv.transpose(0, 2, 3, 1).reshape(-1, d_model)
        n_qkv = qkv_rows.shape[0]
        bias_rows = jnp.concatenate([b_qkv.reshape(-1), b_fc1])
        bias_rows = jnp.pad(bias_rows, (0, 32 * d_model - bias_rows.shape[0])).reshape(32, d_model)
        near, far = fetch(jnp.concatenate([qkv_rows, w_out.reshape(-1, d_model), bias_rows]), y_rank)
        pack1 = jnp.stack([near, far])
        wqkv = pack1[:, :, :n_qkv].reshape(HALVES, HALVES, QKV, hidden, d_model).transpose(0, 2, 1, 3, 4).reshape(-1, d_model)
        wout = pack1[:, :, n_qkv:n_qkv + hidden].reshape(-1, d_model)
        biases = pack1[:, :, n_qkv + hidden:].reshape(HALVES, HALVES, -1)
        bqkv = biases[:, :, :n_qkv].reshape(HALVES, HALVES, QKV, hidden).transpose(0, 2, 1, 3).reshape(-1).astype(F32)
        bfc1 = biases[:, :, n_qkv:n_qkv + ff_local].reshape(2, -1).astype(F32)

        canon = tokens.reshape(TP, n_chunk, c_seq, TP, seq_local)
        ids = jnp.stack([jnp.stack([canon[d, :, :, d ^ k] for k in range(TP)], axis=1) for d in range(TP)])
        ids = xor_order(ids, rank).reshape(TP, rows)
        local_ids = ids - rank * vocab_local
        owned = (local_ids >= 0) & (local_ids < vocab_local)

        def chunk(array, c):
            return lax.slice_in_dim(array, c * c_rows, (c + 1) * c_rows)

        diag_part, x_part, core_part, own_part = gather(emb_local, local_ids[::-1], owned[::-1], TP)
        to_x = swap(diag_part, CORE)
        from_x = [swap(chunk(x_part, c) + chunk(to_x, c), X) for c in range(n_chunk)]
        from_near = own_part + swap(core_part, CORE)
        w1_rows, w2_rows, grad_in = w_fc1.T, w_fc2, grad_y
        w1_near, w1_far = (a.reshape(-1, d_model) for a in fetch(w1_rows, y_rank))
        w2_near, w2_far = (a.reshape(-1, d_model) for a in fetch(w2_rows, y_rank))
        grad_in = grad_in.reshape(TP, n_seq, seq_local, d_model)
        g = [lax.dynamic_index_in_dim(grad_in, rank ^ k, 0, keepdims=False) for k in range(TP)]
        g = [g[0]] + [swap(g[k], k) for k in (1, 2, 3)]
        grad = jnp.stack([a.reshape(n_chunk, c_seq, seq_local, d_model) for a in g], axis=1).reshape(rows, d_model)

        mask_all = attn_mask.reshape(TP, n_seq, seq)
        mask = lax.dynamic_index_in_dim(mask_all, rank, 0, keepdims=False)
        positions = jnp.cumsum(mask, axis=1) * mask + 1
        block_of = jnp.arange(TP) ^ rank
        pos_index = (block_of[:, None] * seq_local + jnp.arange(seq_local)[None]).reshape(seq)
        key_mask = xor_order(mask.reshape(n_seq, TP, seq_local).transpose(1, 0, 2), rank).transpose(1, 0, 2).reshape(n_seq, seq)
        causal = pos_index[:, None] >= pos_index[None, :]
        diagonal = jnp.eye(seq, dtype=bool)
        allowed = (causal & ((key_mask[:, None, :] > 0) | diagonal)).astype(F32)
        allowed_t = (causal.T & ((key_mask[:, :, None] > 0) | diagonal)).astype(F32)

        n_pos = -(-(seq + 2) // 8) * 8
        pos_rel = xor_order(positions.reshape(n_chunk, c_seq, TP, seq_local).transpose(2, 0, 1, 3), rank).transpose(1, 0, 2, 3).reshape(rows)
        one_hot = (pos_rel[:, None] == jnp.arange(n_pos)[None]).astype(BF16)
        pos_rows = dot(one_hot, pos_table[:n_pos], NN)

        is_query = (jnp.arange(3 * n_heads * e) // (2 * hidden)) % 3 == 0
        near_rows = from_near.astype(F32) + pos_rows
        hidden0, normed1, qkv, context = [], [], [], []
        for c in range(n_chunk):
            hidden0.append((chunk(near_rows, c) + from_x[c].astype(F32)).astype(BF16))
            normed1.append(ln_forward(hidden0[c], ln1_gain, ln1_shift))
            projected = dot(normed1[c], wqkv, NT) + bqkv
            qkv.append((projected * jnp.where(is_query, q_scale, 1.0)).astype(BF16).reshape(TP, c_seq, seq_local, -1))
            context.append(attn_forward(allowed, qkv[c], c).reshape(c_rows, -1))
            if c + 1 < n_chunk:
                context[c], from_x[c + 1] = barrier((context[c], from_x[c + 1]))
        w1, w2 = (w1_near, w1_far), (w2_near, w2_far)
        vectors = jnp.stack([b_out, ln2_gain, ln2_shift, b_fc2]).astype(F32)
        out, hidden1, normed2, dpre_near, dpre_far, near, far, d_b_fc1, sum_grad = mlp_forward(hidden0, context, grad, wout, w1, w2, vectors, bfc1)
        near_w2, far_w2 = near, far
        out = out.reshape(n_chunk, TP, c_seq, seq_local, d_model)
        out_rows = jnp.zeros((TP, n_seq, seq_local, d_model), BF16)
        for k in range(TP):
            got = out[:, k].reshape(n_seq, seq_local, d_model)
            got = got if k == 0 else swap(got, k)
            out_rows = lax.dynamic_update_index_in_dim(out_rows, got, rank ^ k, 0)
        out_rows = out_rows.reshape(n_all, seq_local, d_model)

        def start_reduce(near, far, lead=1):
            near = (near + swap(far, CORE).astype(F32)).reshape(lead, HALVES, -1, d_model)
            return near[:, 0], near[:, 1].astype(BF16)

        def end_reduce(own, to_send):
            return (own + swap(to_send, 2).astype(F32)).reshape(-1, d_model)

        g_w2 = start_reduce(near_w2, far_w2)
        d_hidden1, d_context, near, far, near_out, far_out, sums = mlp_backward(context, (dpre_near, dpre_far), normed2, hidden1, grad, w1, wout, vectors[1:2])
        g_w1, g_wout = start_reduce(near, far), start_reduce(near_out, far_out)
        d_context = d_context.reshape(n_chunk, TP, c_seq, seq_local, -1)
        d_b_qkv, d_hidden0, d_ln1_gain, d_ln1_shift, near, far = 0.0, [], 0.0, 0.0, 0.0, 0.0
        for c in range(n_chunk):
            d_qkv, d_bias = attn_backward(allowed_t, qkv[c], d_context, c, q_scale)
            d_b_qkv = d_b_qkv + d_bias[ROWS]
            d_qkv = d_qkv.reshape(c_rows, -1)
            d_norm1 = dot(d_qkv, wqkv, NN, BF16)
            d_hidden0_ln, d_gain, d_shift = ln_backward(hidden0[c], ln1_gain, d_norm1)
            d_ln1_gain, d_ln1_shift = d_ln1_gain + d_gain, d_ln1_shift + d_shift
            d_hidden0.append((chunk(d_hidden1, c).astype(F32) + d_hidden0_ln).astype(BF16))
            if c + 1 < n_chunk:
                d_hidden0[c], d_context = barrier((d_hidden0[c], d_context))
            width = 6 * hidden
            near = near + dot(d_qkv[:, :width], normed1[c], TN)
            far = far + dot(d_qkv[:, width:], normed1[c], TN)
        g_wqkv = start_reduce(near, far.astype(BF16), 3)

        d_pos = sum(dot(chunk(one_hot, c), d_hidden0[c], TN) for c in range(n_chunk))
        vectors = jnp.stack([d_ln1_gain, d_ln1_shift, sums[2], sums[0], sums[1], sum_grad[0]])
        hid_b = d_b_qkv.reshape(HALVES, QKV, HALVES, hidden).transpose(0, 2, 1, 3).reshape(TP, -1)
        block_b = jnp.concatenate([hid_b, d_b_fc1[:2].reshape(TP, -1)], axis=1)
        block_b = jnp.stack([block_b[0], block_b[2], block_b[1], block_b[3]])
        block_b = xor_order(block_b, rank)
        small = jnp.concatenate([vectors.reshape(-1), block_b.reshape(-1)])
        small = jnp.pad(small, (0, -small.shape[0] % (16 * d_model))).reshape(-1, d_model)
        total = jnp.concatenate([d_pos, small])
        total = total + swap(total, CORE)

        own_ids = jnp.where(owned, local_ids, vocab_local)
        x_rows = [swap(d_hidden0[c], X) for c in range(n_chunk)]
        total = total + swap(total, X)
        all_rows = d_hidden0 + [swap(a, CORE) for a in d_hidden0] + x_rows + [swap(a, CORE) for a in x_rows]
        d_emb = scatter(own_ids.reshape(-1), repeats(own_ids, vocab_local), all_rows, vocab_local)
        d_pos = jnp.pad(total[:n_pos], ((0, pos_table.shape[0] - n_pos), (0, 0)))
        vectors = total[n_pos:n_pos + 6]
        blocks = total[n_pos + 6:].reshape(-1)[:block_b.size].reshape(block_b.shape)
        own_b = lax.dynamic_index_in_dim(blocks, rank, 0, keepdims=False)
        d_w_qkv = end_reduce(*g_wqkv).reshape(3, local_heads, e, d_model).transpose(0, 3, 1, 2)
        d_w_out, d_w_fc1, d_w_fc2 = (end_reduce(*a) for a in (g_wout, g_w1, g_w2))
        return (out_rows, d_emb, d_pos, vectors[0], vectors[1], d_w_qkv, own_b[:3 * hidden].reshape(3, local_heads, e), d_w_out.reshape(local_heads, e, d_model), vectors[2], vectors[3], vectors[4], d_w_fc1.T, own_b[3 * hidden:], d_w_fc2, vectors[5])

    vec, part, heads = P(None), P('tp', None), P(None, 'tp', None)
    in_specs = (P('dp', None), P('dp', None), part, P(None, None), vec, vec, P(None, None, 'tp', None), heads, P('tp', None, None), vec, vec, vec, P(None, 'tp'), P('tp'), part, vec, P('dp', 'tp', None))
    sums, split = P('dp'), P(('dp', 'tp'), None)
    out_specs = (P('dp', 'tp', None), split, P('dp', None), sums, sums, P('dp', None, 'tp', None), P('dp', 'tp', None), P(('dp', 'tp'), None, None), sums, sums, sums, P('dp', 'tp'), P(('dp', 'tp')), split, sums)
    return jax.shard_map(device_body, mesh=mesh, in_specs=in_specs, out_specs=out_specs, check_vma=False)
```
